32 devices in a mesh: rep: 4 (over z), own: 8 (over y, x, core).
Axes of the slice: x: 2, y: 2, z: 4, core: 2. Of those that a mesh axis runs over, the one named last changes fastest.
Arguments:
- grads: float32 [16, 576, 1024], P('rep', 'own'), may hold values from -60 to 60
- momentum: bfloat16 [32, 576, 1024], P(('rep', 'own')), may hold values from -6 to 6
- owner_table: int32 [4, 8], replicated, may hold values from 0 to 7, each once within a row
Outputs:
- new_momentum: bfloat16 [32, 576, 1024], P(('rep', 'own'))
- updates: bfloat16 [16, 576, 1024], P(None, 'own')
The draws below stay inside these ranges and needn't reach their ends.
Inputs may be any that keep to these rules, and one draw needn't show every extreme that they name: Each row of owner_table is a permutation of 0 to 7; entries of 4 or more mark empty slots.
All inputs are finite; a program needn't handle non-finite values.
Results may differ from the reference program's by a relative error of at most 0.01.
Values may be sent and summed in bfloat16 or wider, within the bound.
No kernel may reach another device: no remote copies, remote signals or barrier semaphores. Data moves between devices by JAX's collectives and lax.ppermute only.
A program may use at most 128 MiB of HBM per device.

```python
import math
import jax
import jax.numpy as jnp
from jax import lax

MR = 576
MC = 1024
ITERS = 2
MATS = 4
MATS_ALL = 16
SLOTS = 32
N_REP = 4
N_OWN = 8


def draw_grads(key, part):
    keys = jax.random.split(jax.random.fold_in(key, 7), 3)
    base = jnp.clip(jax.random.normal(keys[0], (MATS_ALL, MR, MC), jnp.float32), -6.0, 6.0)
    row_scale = jnp.exp(jax.random.uniform(keys[1], (MATS_ALL, MR, 1), jnp.float32) * math.log(10.0))
    col_scale = jnp.exp(jax.random.uniform(keys[2], (MATS_ALL, 1, MC), jnp.float32) * math.log(10.0))
    return base * row_scale * col_scale * 0.1


def shard_levels(key, shape, pieces, smallest, top_value):
    gain, own = 1.0, jax.random.fold_in(key, 6)
    for axis_at, blocks in pieces:
        heights = jnp.exp(jax.random.uniform(jax.random.fold_in(own, axis_at), (blocks,), jnp.float32, smallest / len(pieces), top_value / len(pieces)))
        gain = gain * jnp.repeat(heights, shape[axis_at] // blocks).reshape([-1 if axis == axis_at else 1 for axis in range(len(shape))])
    return gain


def gaussian(key, extent, spread, bound, pieces=(), kind=jnp.bfloat16):
    loudness = shard_levels(key, extent, pieces, -0.22, 0.18) if pieces else 1.0
    values = jax.random.normal(key, extent, jnp.float32) * spread * loudness
    return jnp.minimum(jnp.maximum(values, -bound), bound).astype(kind)


def setup_inputs(seed: int = 0) -> dict:
    key_list = jax.random.split(jax.random.key(seed), 4)
    return {
        "grads": draw_grads(jax.random.fold_in(key_list[3], 71), 0),
        "momentum": gaussian(key_list[1], (SLOTS, MR, MC), 1.0, 6.0, ((0, 32),)),
        "owner_table": jax.vmap(lambda own: jax.random.permutation(own, N_OWN))(jax.random.split(key_list[2], N_REP)).reshape((N_REP, N_OWN)).astype(jnp.int32),
    }


DECAY = 0.95
COEF_A = 3.4445
COEF_B = -4.775
COEF_C = 2.0315
EPSILON = 1e-07

def orthogonalize(blend):
    total = jnp.sqrt(jnp.sum(blend * blend))
    iterate = (blend / (total + EPSILON)).astype(jnp.bfloat16)
    factor = 0.2 * math.sqrt(max(MR, MC))
    result = None
    for turn in range(ITERS):
        gram = jnp.dot(iterate, iterate.T, preferred_element_type=jnp.float32).astype(jnp.bfloat16)
        square = jnp.dot(gram, gram, preferred_element_type=jnp.float32)
        poly = (COEF_B * gram.astype(jnp.float32) + COEF_C * square).astype(jnp.bfloat16)
        mixed = COEF_A * iterate.astype(jnp.float32) + jnp.dot(poly, iterate, preferred_element_type=jnp.float32)
        if turn + 1 < ITERS:
            iterate = mixed.astype(jnp.bfloat16)
        else:
            result = (factor * mixed).astype(jnp.bfloat16)
    return result

def reference(grads, momentum, owner_table):
    half_grads = grads.astype(jnp.bfloat16)
    is_live = (owner_table < MATS).reshape(-1)
    clamped = jnp.minimum(owner_table, MATS - 1).astype(jnp.int32)
    source = (jnp.arange(N_REP, dtype=jnp.int32)[:, None] * MATS + clamped).reshape(-1).astype(jnp.int32)

    def slot_step(inputs):
        held, index, flag = inputs
        gradient = jnp.where(flag, half_grads[index].astype(jnp.float32), jnp.zeros((MR, MC), jnp.float32))
        return (DECAY * held.astype(jnp.float32) + gradient).astype(jnp.bfloat16)
    new_momentum = lax.map(slot_step, (momentum, source, is_live))
    inverse = jnp.argsort(owner_table, axis=1)[:, :MATS].astype(jnp.int32)
    slot_of = (jnp.arange(N_REP, dtype=jnp.int32)[:, None] * N_OWN + inverse).reshape(-1).astype(jnp.int32)

    def matrix_step(inputs):
        gradient_half, slot = inputs
        gradient = gradient_half.astype(jnp.float32)
        moment = DECAY * momentum[slot].astype(jnp.float32) + gradient
        return orthogonalize(gradient + DECAY * moment)
    updates = lax.map(matrix_step, (half_grads, slot_of))
    return (new_momentum, updates)
```

```python
import functools
import math

import jax
import jax.numpy as jnp
from jax import lax
from jax.experimental import pallas as pl
from jax.experimental.pallas import tpu as pltpu
from jax.sharding import PartitionSpec as P


ITERS = 2
CHUNKS = 2

DECAY = 0.95
COEF_A = 3.4445
COEF_B = -4.775
COEF_C = 2.0315
EPSILON = 1e-07


VMEM = pl.BlockSpec(memory_space=pltpu.VMEM)
SMEM = pl.BlockSpec(memory_space=pltpu.SMEM)
ANY = pl.BlockSpec(memory_space=pl.ANY)


def limit(mib):
    return pltpu.CompilerParams(vmem_limit_bytes=mib * 2**20)


def near(x):
    return pltpu.with_memory_space_constraint(x, pltpu.VMEM)


def far(x):
    return pltpu.with_memory_space_constraint(x, pltpu.HBM)


def orthogonalize(blend):
    total = jnp.sqrt(jnp.sum(blend * blend))
    iterate = (blend / (total + EPSILON)).astype(jnp.bfloat16)
    factor = 0.2 * math.sqrt(max(blend.shape[0], blend.shape[1]))
    result = None
    for turn in range(ITERS):
        gram = jnp.dot(iterate, iterate.T, preferred_element_type=jnp.float32).astype(jnp.bfloat16)
        square = jnp.dot(gram, gram, preferred_element_type=jnp.float32)
        poly = (COEF_B * gram.astype(jnp.float32) + COEF_C * square).astype(jnp.bfloat16)
        mixed = COEF_A * iterate.astype(jnp.float32) + jnp.dot(
            poly, iterate, preferred_element_type=jnp.float32
        )
        if turn + 1 < ITERS:
            iterate = mixed.astype(jnp.bfloat16)
        else:
            result = (factor * mixed).astype(jnp.bfloat16)
    return result


def general_body(grads, momentum, owner_table):
    group = lax.axis_index("rep")
    slot_matrix = lax.dynamic_index_in_dim(owner_table, group, 0, keepdims=False)
    matrix_count, _, _ = grads.shape
    is_live = slot_matrix < matrix_count
    clamped = jnp.minimum(slot_matrix, matrix_count - 1)
    half_grads = grads.astype(jnp.bfloat16)
    outgoing = jnp.take(half_grads, clamped, axis=0) * is_live[:, None, None].astype(jnp.bfloat16)
    incoming = lax.all_to_all(outgoing, "own", split_axis=0, concat_axis=1, tiled=True)
    gradient = incoming[0].astype(jnp.float32)
    moment = DECAY * momentum[0].astype(jnp.float32) + gradient
    new_momentum = moment.astype(jnp.bfloat16)[None]
    update = orthogonalize(gradient + DECAY * moment)
    returned = lax.all_to_all(update[None], "own", split_axis=1, concat_axis=0, tiled=True)
    holders = jnp.argsort(slot_matrix)[:matrix_count]
    grouped = jnp.take(returned, holders, axis=0)
    updates = lax.all_gather(grouped, "rep", axis=0, tiled=True)
    return (new_momentum, updates)


def send_order(own):
    if own == 8:
        return [6, 7, 2, 4, 3, 5, 1]
    return list(range(own - 1, 0, -1))


def partner(kind, z, reps):
    other = z ^ 1 if kind == 0 else z + 1 if z % 2 else z - 1
    return other if 0 <= other < reps else None


def line_pairs(kind, reps, own):
    pairs = []
    for z in range(reps):
        other = partner(kind, z, reps)
        for o in range(own):
            pairs.append((z * own + o, (z if other is None else other) * own + (o ^ (other is None))))
    return pairs


def source_of(stream, step, z):
    return z + step * (1 - 2 * ((z + stream + step + 1) % 2))


def line_steps(reps):
    return [
        (stream, step)
        for step in range(1, reps)
        for stream in (0, 1)
        if any(0 <= source_of(stream, step, z) < reps for z in range(reps))
    ]


def pack_kernel(table_hbm, grads_hbm, *refs):
    *outs, table, grads, table_sem, sems = refs
    group, me = lax.axis_index("rep"), lax.axis_index("own")
    count = grads.shape[0]
    flights = [pltpu.make_async_copy(table_hbm, table, table_sem)]
    flights += [pltpu.make_async_copy(grads_hbm.at[k], grads.at[k], sems.at[k]) for k in range(count)]
    for flight in flights:
        flight.start()
    for flight in flights:
        flight.wait()
    for d, out in enumerate(outs):
        matrix = table[group, me ^ d]

        @pl.when(matrix < count)
        def _():
            out[...] = grads[jnp.minimum(matrix, count - 1)].astype(jnp.bfloat16)

        @pl.when(matrix >= count)
        def _():
            out[...] = jnp.zeros(out.shape, out.dtype)


def mix_block(me, d, at, block, momentum, staged, stage_at, new_momentum, sem, blend):
    rows, columns = block.shape
    gradient = block[...].astype(jnp.float32)
    moment = DECAY * momentum[me ^ d].astype(jnp.float32) + gradient
    staged[stage_at] = moment.astype(jnp.bfloat16)
    flight = pltpu.make_async_copy(staged.at[stage_at], new_momentum.at[me ^ d], sem)
    flight.start()
    mix = gradient + DECAY * moment
    blend[at * rows : (at + 1) * rows, :] = mix.astype(jnp.bfloat16)
    return jnp.sum((mix * mix).reshape(rows // 8, 8, columns), axis=0), flight


def mix_kernel(order, *refs):
    blocks, momentum = refs[: len(order)], refs[len(order)]
    new_momentum, blend, squares = refs[len(order) + 1 : len(order) + 4]
    staged, sems = refs[-2:]
    me = lax.axis_index("own")
    total, flights = jnp.zeros(squares.shape, jnp.float32), []
    for i, d in enumerate(order):
        part, flight = mix_block(me, d, i, blocks[i], momentum, staged, i, new_momentum, sems.at[i], blend)
        total += part
        flights.append(flight)
    squares[...] = total
    for flight in flights:
        flight.wait()


def update_kernel(order, first, chunks, *refs):
    late = order[first:]
    blocks, refs = refs[: len(late)], refs[len(late) :]
    momentum, squares = refs[0], refs[3]
    new_momentum, blend = refs[4:6]
    outs = refs[6 : 6 + len(order) * chunks]
    iterate, staged, sems = refs[-3:]
    me = lax.axis_index("own")
    rows, columns = blocks[0].shape
    width = columns // chunks
    sums, flights = squares[...], []
    for i, d in enumerate(late):
        part, flight = mix_block(me, d, first + i, blocks[i], momentum, staged, i, new_momentum, sems.at[i], blend)
        sums += part
        flights.append(flight)
    scale = 1.0 / (jnp.sqrt(jnp.sum(sums, keepdims=True)) + EPSILON)
    factor = 0.2 * math.sqrt(max(rows * len(order), columns))
    for turn in range(ITERS):
        y = blend[...] if turn == 0 else iterate[...]
        gram32 = lax.dot_general(y, y, (((1,), (1,)), ((), ())), preferred_element_type=jnp.float32)
        if turn == 0:
            gram32 = gram32 * (scale * scale)
        gram = gram32.astype(jnp.bfloat16)
        square = jnp.dot(gram, gram, preferred_element_type=jnp.float32)
        poly = (COEF_B * gram.astype(jnp.float32) + COEF_C * square).astype(jnp.bfloat16)
        final = turn + 1 == ITERS
        for c in range(chunks):
            part = y[:, c * width : (c + 1) * width]
            mixed = COEF_A * part.astype(jnp.float32) + jnp.dot(poly, part, preferred_element_type=jnp.float32)
            if turn == 0:
                mixed = mixed * scale
            if final:
                scaled = (factor * mixed).astype(jnp.bfloat16)
                for i, d in enumerate(order):
                    outs[c * len(order) + d][...] = scaled[i * rows : (i + 1) * rows, :]
            else:
                iterate[:, c * width : (c + 1) * width] = mixed.astype(jnp.bfloat16)
    for flight in flights:
        flight.wait()


def group_kernel(own, table, *refs):
    parts, out = refs[:own], refs[own]
    group, me = lax.axis_index("rep"), lax.axis_index("own")
    for d in range(own):
        matrix = table[group, me ^ d]

        @pl.when(matrix < out.shape[0])
        def _():
            out[matrix] = parts[d][...]


def place_kernel(reps, where, *refs):
    parts, out, sems = refs[: len(where)], refs[-2], refs[-1]
    group = lax.axis_index("rep")
    count, _, width = parts[0].shape
    flights = []
    for i, (c, stream, step) in enumerate(where):
        source = group + step * (1 - 2 * lax.rem(group + stream + step + 1, 2))
        here = (source >= 0) & (source < reps)
        at = jnp.clip(source, 0, reps - 1) * count
        to = out.at[pl.ds(at, count), :, pl.ds(c * width, width)]
        flights.append((here, pltpu.make_async_copy(parts[i], to, sems.at[i])))
    for here, copy in flights:
        pl.when(here)(copy.start)
    for here, copy in flights:
        pl.when(here)(copy.wait)


def place(reps, where, parts, shape, out):
    aliases = {} if out is None else {len(where): 0}
    return pl.pallas_call(
        functools.partial(place_kernel, reps, where),
        in_specs=[VMEM] * len(where) + [ANY] * len(aliases),
        out_specs=ANY,
        out_shape=jax.ShapeDtypeStruct(shape, jnp.bfloat16),
        input_output_aliases=aliases,
        scratch_shapes=[pltpu.SemaphoreType.DMA((len(where),))],
        compiler_params=limit(4),
    )(*map(near, parts), *([] if out is None else [out]))


def chunked_body(own, reps, grads, momentum, owner_table):
    count, rows, columns = grads.shape
    width = columns // CHUNKS
    half = jnp.bfloat16
    order = send_order(own)
    arrival = [0, order[-1]] + order[:-1]
    first = own // 2

    def swap(x, d):
        return lax.ppermute(x, "own", [(i, i ^ d) for i in range(own)])

    outgoing = pl.pallas_call(
        pack_kernel,
        in_specs=[ANY, ANY],
        out_specs=[VMEM] * own,
        out_shape=[pltpu.VMEM((rows, columns), half)] * own,
        scratch_shapes=[
            pltpu.SMEM(owner_table.shape, jnp.int32),
            pltpu.VMEM(grads.shape, grads.dtype),
            pltpu.SemaphoreType.DMA(()),
            pltpu.SemaphoreType.DMA((count,)),
        ],
        compiler_params=limit(8),
        name="pack",
    )(far(owner_table), far(grads))
    incoming = {0: outgoing[0]}
    for d in order:
        incoming[d] = swap(outgoing[d], d)
    slots = near(momentum.reshape(own, rows, columns))
    new_momentum, blend, squares = pl.pallas_call(
        functools.partial(mix_kernel, arrival[:first]),
        in_specs=[VMEM] * (first + 1),
        out_specs=[ANY, VMEM, VMEM],
        out_shape=[
            jax.ShapeDtypeStruct((own, rows, columns), half),
            pltpu.VMEM((own * rows, columns), half),
            pltpu.VMEM((8, columns), jnp.float32),
        ],
        scratch_shapes=[pltpu.VMEM((first, rows, columns), half), pltpu.SemaphoreType.DMA((first,))],
        compiler_params=limit(8),
        name="mix",
    )(*[near(incoming[d]) for d in arrival[:first]], slots)
    late = own - first
    new_momentum, _, *parts = pl.pallas_call(
        functools.partial(update_kernel, arrival, first, CHUNKS),
        in_specs=[VMEM] * (late + 1) + [ANY, VMEM, VMEM],
        out_specs=[ANY] + [VMEM] * (1 + own * CHUNKS),
        out_shape=[
            jax.ShapeDtypeStruct((own, rows, columns), half),
            pltpu.VMEM((own * rows, columns), half),
        ]
        + [pltpu.VMEM((rows, width), half)] * (own * CHUNKS),
        input_output_aliases={late + 1: 0, late + 2: 1},
        scratch_shapes=[
            pltpu.VMEM((own * rows, columns), half),
            pltpu.VMEM((late, rows, columns), half),
            pltpu.SemaphoreType.DMA((late,)),
        ],
        compiler_params=limit(24),
        name="update",
    )(*[near(incoming[d]) for d in arrival[first:]], slots, new_momentum, near(blend), near(squares))
    held = {}
    for c in range(CHUNKS):
        back = [parts[c * own]] + [None] * (own - 1)
        for d in order:
            back[d] = swap(parts[c * own + d], d)
        held[c, 0, 0] = pl.pallas_call(
            functools.partial(group_kernel, own),
            in_specs=[SMEM] + [VMEM] * own,
            out_specs=VMEM,
            out_shape=pltpu.VMEM((count, rows, width), half),
            compiler_params=limit(4),
        )(owner_table, *map(near, back))
    pairs = [line_pairs(kind, reps, own) for kind in (0, 1)]
    steps = line_steps(reps)
    for stream, step in steps:
        for c in range(CHUNKS):
            behind = held[c, 0, 0] if step == 1 else held[c, stream, step - 1]
            held[c, stream, step] = lax.ppermute(behind, ("rep", "own"), pairs[(stream + step + 1) % 2])
    shape = (reps * count, rows, columns)
    last = [key for key in held if key[1:] == steps[-1]]
    soon = [key for key in held if key not in last]
    updates = place(reps, soon, [held[key] for key in soon], shape, None)
    updates = place(reps, last, [held[key] for key in last], shape, updates)
    return (new_momentum.reshape(1, own * rows, columns), updates)


def solution(mesh):
    in_specs = (P("rep", "own", None), P(("rep", "own"), None, None), P())
    out_specs = (P(("rep", "own"), None, None), P(None, "own", None))
    own, reps = mesh.shape["own"], mesh.shape["rep"]

    def step(grads, momentum, owner_table):
        _, total_rows, columns = grads.shape
        tiled = total_rows % (8 * own) == 0 and columns % (128 * CHUNKS) == 0
        if not tiled or own & (own - 1) or not 4 <= own <= 8 or reps < 2:
            return jax.shard_map(general_body, mesh=mesh, in_specs=in_specs, out_specs=out_specs, check_vma=False)(
                grads, momentum, owner_table
            )

        def body(*args):
            return chunked_body(own, reps, *args)

        mapped = jax.shard_map(body, mesh=mesh, in_specs=in_specs, out_specs=out_specs, check_vma=False)
        return mapped(grads, momentum, owner_table)

    return step
```

```python
import functools
import math

import jax
import jax.numpy as jnp
from jax import lax
from jax.experimental import pallas as pl
from jax.experimental.pallas import tpu as pltpu
from jax.sharding import PartitionSpec as P


ITERS = 2
EDGES = (0, 4, 8)
CHUNKS = len(EDGES) - 1
SOON = 1
PAIRED = ((6,), (2, 4))

DECAY = 0.95
COEF_A = 3.4445
COEF_B = -4.775
COEF_C = 2.0315
EPSILON = 1e-07

ORDER = (6, 7, 2, 4, 3, 5, 1)


VMEM = pl.BlockSpec(memory_space=pltpu.VMEM)
SMEM = pl.BlockSpec(memory_space=pltpu.SMEM)
ANY = pl.BlockSpec(memory_space=pl.ANY)


def limit(mib):
    return pltpu.CompilerParams(vmem_limit_bytes=mib * 2**20)


def spans(columns):
    unit = columns // EDGES[-1]
    return [(unit * a, unit * b) for a, b in zip(EDGES, EDGES[1:])]


def near(x):
    return pltpu.with_memory_space_constraint(x, pltpu.VMEM)


def far(x):
    return pltpu.with_memory_space_constraint(x, pltpu.HBM)


def orthogonalize(blend):
    total = jnp.sqrt(jnp.sum(blend * blend))
    iterate = (blend / (total + EPSILON)).astype(jnp.bfloat16)
    factor = 0.2 * math.sqrt(max(blend.shape[0], blend.shape[1]))
    result = None
    for turn in range(ITERS):
        gram = jnp.dot(iterate, iterate.T, preferred_element_type=jnp.float32).astype(jnp.bfloat16)
        square = jnp.dot(gram, gram, preferred_element_type=jnp.float32)
        poly = (COEF_B * gram.astype(jnp.float32) + COEF_C * square).astype(jnp.bfloat16)
        mixed = COEF_A * iterate.astype(jnp.float32) + jnp.dot(
            poly, iterate, preferred_element_type=jnp.float32
        )
        if turn + 1 < ITERS:
            iterate = mixed.astype(jnp.bfloat16)
        else:
            result = (factor * mixed).astype(jnp.bfloat16)
    return result


def general_body(grads, momentum, owner_table):
    group = lax.axis_index("rep")
    slot_matrix = lax.dynamic_index_in_dim(owner_table, group, 0, keepdims=False)
    matrix_count, _, _ = grads.shape
    is_live = slot_matrix < matrix_count
    clamped = jnp.minimum(slot_matrix, matrix_count - 1)
    half_grads = grads.astype(jnp.bfloat16)
    outgoing = jnp.take(half_grads, clamped, axis=0) * is_live[:, None, None].astype(jnp.bfloat16)
    incoming = lax.all_to_all(outgoing, "own", split_axis=0, concat_axis=1, tiled=True)
    gradient = incoming[0].astype(jnp.float32)
    moment = DECAY * momentum[0].astype(jnp.float32) + gradient
    new_momentum = moment.astype(jnp.bfloat16)[None]
    update = orthogonalize(gradient + DECAY * moment)
    returned = lax.all_to_all(update[None], "own", split_axis=1, concat_axis=0, tiled=True)
    holders = jnp.argsort(slot_matrix)[:matrix_count]
    grouped = jnp.take(returned, holders, axis=0)
    updates = lax.all_gather(grouped, "rep", axis=0, tiled=True)
    return (new_momentum, updates)


def send_order(own):
    return [d for d in ORDER if d < own]


def parcels(own, chunks):
    return [(c, d) for c in chunks for d in range(own) if d & -2 == d or d & -2 not in PAIRED[c]]


def partner(kind, z, reps):
    other = z ^ 1 if kind == 0 else z + 1 if z % 2 else z - 1
    return other if 0 <= other < reps else None


def line_pairs(kind, reps, own):
    pairs = []
    for z in range(reps):
        other = partner(kind, z, reps)
        for o in range(own):
            pairs.append((z * own + o, (z if other is None else other) * own + (o ^ (other is None))))
    return pairs


def source_of(stream, step, z):
    return z + step * (1 - 2 * ((z + stream + step + 1) % 2))


def line_steps(reps):
    return [
        (stream, step)
        for step in range(1, reps)
        for stream in (0, 1)
        if any(0 <= source_of(stream, step, z) < reps for z in range(reps))
    ]


def pack_kernel(table_hbm, grads_hbm, *refs):
    *outs, table, grads, table_sem, sems = refs
    group, me = lax.axis_index("rep"), lax.axis_index("own")
    count = grads.shape[0]
    flights = [pltpu.make_async_copy(table_hbm, table, table_sem)]
    flights += [pltpu.make_async_copy(grads_hbm.at[k], grads.at[k], sems.at[k]) for k in range(count)]
    for flight in flights:
        flight.start()
    for flight in flights:
        flight.wait()
    for d, out in enumerate(outs):
        matrix = table[group, me ^ d]

        @pl.when(matrix < count)
        def _():
            out[...] = grads[jnp.minimum(matrix, count - 1)].astype(jnp.bfloat16)

        @pl.when(matrix >= count)
        def _():
            out[...] = jnp.zeros(out.shape, out.dtype)


def mix_block(me, d, at, block, momentum, staged, stage_at, new_momentum, sem, blend):
    rows, columns = block.shape
    gradient = block[...].astype(jnp.float32)
    moment = DECAY * momentum[me ^ d].astype(jnp.float32) + gradient
    staged[stage_at] = moment.astype(jnp.bfloat16)
    flight = pltpu.make_async_copy(staged.at[stage_at], new_momentum.at[me ^ d], sem)
    flight.start()
    mix = gradient + DECAY * moment
    blend[at * rows : (at + 1) * rows, :] = mix.astype(jnp.bfloat16)
    return jnp.sum((mix * mix).reshape(rows // 8, 8, columns), axis=0), flight


def mix_kernel(order, first, last, *refs):
    blocks, momentum = refs[: last - first], refs[last - first]
    new_momentum, blend, squares, staged, sems = refs[-5:]
    before = refs[last - first + 3] if first else None
    me = lax.axis_index("own")
    total, flights = (before[...] if first else jnp.zeros(squares.shape, jnp.float32)), []
    for i in range(last - first):
        part, flight = mix_block(
            me, order[first + i], first + i, blocks[i], momentum, staged, i, new_momentum, sems.at[i], blend
        )
        total += part
        flights.append(flight)
    squares[...] = total
    for flight in flights:
        flight.wait()


def finish_chunks(order, chunks, poly, y, at, outs):
    me = lax.axis_index("own")
    rows, edges = y.shape[0] // len(order), spans(y.shape[1])
    factor = 0.2 * math.sqrt(max(y.shape))
    for c in chunks:
        part = y[:, edges[c][0] : edges[c][1]]
        mixed = COEF_A * part.astype(jnp.float32) + jnp.dot(poly, part, preferred_element_type=jnp.float32)
        scaled = (factor * mixed).astype(jnp.bfloat16)
        for i, d in enumerate(order):
            piece = scaled[i * rows : (i + 1) * rows, :]
            if d & -2 in PAIRED[c]:
                outs[at[c, d & -2]][(me ^ d) & 1] = piece
            else:
                outs[at[c, d]][...] = piece


def update_kernel(order, first, *refs):
    late = order[first:]
    blocks, refs = refs[: len(late)], refs[len(late) :]
    momentum, squares = refs[0], refs[3]
    new_momentum, blend, iterate = refs[4:7]
    outs = refs[7 + (SOON < CHUNKS) : -2]
    staged, sems = refs[-2:]
    me = lax.axis_index("own")
    sums, flights = squares[...], []
    for i, d in enumerate(late):
        part, flight = mix_block(me, d, first + i, blocks[i], momentum, staged, i, new_momentum, sems.at[i], blend)
        sums += part
        flights.append(flight)
    scale = 1.0 / (jnp.sqrt(jnp.sum(sums, keepdims=True)) + EPSILON)
    for turn in range(ITERS):
        y = blend[...] if turn == 0 else iterate[...]
        gram32 = lax.dot_general(y, y, (((1,), (1,)), ((), ())), preferred_element_type=jnp.float32)
        if turn == 0:
            gram32 = gram32 * (scale * scale)
        gram = gram32.astype(jnp.bfloat16)
        square = jnp.dot(gram, gram, preferred_element_type=jnp.float32)
        poly = (COEF_B * gram.astype(jnp.float32) + COEF_C * square).astype(jnp.bfloat16)
        if turn + 1 < ITERS:
            for start, stop in spans(y.shape[1]):
                part = y[:, start:stop]
                mixed = COEF_A * part.astype(jnp.float32) + jnp.dot(poly, part, preferred_element_type=jnp.float32)
                if turn == 0:
                    mixed = mixed * scale
                iterate[:, start:stop] = mixed.astype(jnp.bfloat16)
    if SOON < CHUNKS:
        refs[7][...] = poly
    soon = range(SOON)
    finish_chunks(order, soon, poly, iterate, {key: i for i, key in enumerate(parcels(len(order), soon))}, outs)
    for flight in flights:
        flight.wait()


def rest_kernel(order, poly, iterate, *outs):
    chunks = range(SOON, CHUNKS)
    at = {key: i for i, key in enumerate(parcels(len(order), chunks))}
    finish_chunks(order, chunks, poly[...], iterate, at, outs)


def group_kernel(table, *refs):
    *parts, out = refs
    group, me = lax.axis_index("rep"), lax.axis_index("own")
    for d, part in enumerate(parts):
        matrix = table[group, me ^ d]

        @pl.when(matrix < out.shape[0])
        def _():
            out[matrix] = part[me & 1] if len(part.shape) == 3 else part[...]


def place_kernel(reps, where, *refs):
    parts, out, sems = refs[: len(where)], refs[-2], refs[-1]
    group = lax.axis_index("rep")
    count = parts[0].shape[0]
    at_columns = spans(out.shape[2])
    flights = []
    for i, (c, stream, step) in enumerate(where):
        source = group + step * (1 - 2 * lax.rem(group + stream + step + 1, 2))
        here = (source >= 0) & (source < reps)
        at = jnp.clip(source, 0, reps - 1) * count
        start, stop = at_columns[c]
        to = out.at[pl.ds(at, count), :, pl.ds(start, stop - start)]
        flights.append((here, pltpu.make_async_copy(parts[i], to, sems.at[i])))
    for here, copy in flights:
        pl.when(here)(copy.start)
    for here, copy in flights:
        pl.when(here)(copy.wait)


def place(reps, where, parts, shape, out):
    aliases = {} if out is None else {len(where): 0}
    return pl.pallas_call(
        functools.partial(place_kernel, reps, where),
        in_specs=[VMEM] * len(where) + [ANY] * len(aliases),
        out_specs=ANY,
        out_shape=jax.ShapeDtypeStruct(shape, jnp.bfloat16),
        input_output_aliases=aliases,
        scratch_shapes=[pltpu.SemaphoreType.DMA((len(where),))],
        compiler_params=limit(4),
    )(*map(near, parts), *([] if out is None else [out]))


def chunked_body(own, reps, grads, momentum, owner_table):
    count, rows, columns = grads.shape
    widths = [b - a for a, b in spans(columns)]
    half = jnp.bfloat16
    order = send_order(own)
    arrival = [0, order[-1]] + order[:-1]
    stages = [0, own // 2, own - 2] if own > 4 else [0, own - 2]

    def swap(x, d):
        return lax.ppermute(x, "own", [(i, i ^ d) for i in range(own)])

    outgoing = pl.pallas_call(
        pack_kernel,
        in_specs=[ANY, ANY],
        out_specs=[VMEM] * own,
        out_shape=[pltpu.VMEM((rows, columns), half)] * own,
        scratch_shapes=[
            pltpu.SMEM(owner_table.shape, jnp.int32),
            pltpu.VMEM(grads.shape, grads.dtype),
            pltpu.SemaphoreType.DMA(()),
            pltpu.SemaphoreType.DMA((count,)),
        ],
        compiler_params=limit(8),
        name="pack",
    )(far(owner_table), far(grads))
    incoming = {0: outgoing[0]}
    for d in order:
        incoming[d] = swap(outgoing[d], d)
    slots = near(momentum.reshape(own, rows, columns))
    state = []
    for first, last in zip(stages, stages[1:]):
        aliases = {last - first + 1: 0, last - first + 2: 1} if first else {}
        state = pl.pallas_call(
            functools.partial(mix_kernel, arrival, first, last),
            in_specs=[VMEM] * (last - first + 1) + ([ANY, VMEM, VMEM] if first else []),
            out_specs=[ANY, VMEM, VMEM],
            out_shape=[
                jax.ShapeDtypeStruct((own, rows, columns), half),
                pltpu.VMEM((own * rows, columns), half),
                pltpu.VMEM((8, columns), jnp.float32),
            ],
            input_output_aliases=aliases,
            scratch_shapes=[pltpu.VMEM((last - first, rows, columns), half), pltpu.SemaphoreType.DMA((last - first,))],
            compiler_params=limit(8),
        )(*[near(incoming[d]) for d in arrival[first:last]], slots, *state)
        state = [state[0], near(state[1]), near(state[2])]
    first = stages[-1]
    late = own - first
    shapes = {
        (c, d): pltpu.VMEM((2,) * (d in PAIRED[c]) + (rows, widths[c]), half) for c, d in parcels(own, range(CHUNKS))
    }
    now, rest = parcels(own, range(SOON)), parcels(own, range(SOON, CHUNKS))
    new_momentum, _, iterate, *parts = pl.pallas_call(
        functools.partial(update_kernel, arrival, first),
        in_specs=[VMEM] * (late + 1) + [ANY, VMEM, VMEM],
        out_specs=[ANY] + [VMEM] * (2 + bool(rest) + len(now)),
        out_shape=[
            jax.ShapeDtypeStruct((own, rows, columns), half),
            pltpu.VMEM((own * rows, columns), half),
            pltpu.VMEM((own * rows, columns), half),
        ]
        + [pltpu.VMEM((own * rows, own * rows), half)] * bool(rest)
        + [shapes[key] for key in now],
        input_output_aliases={late + 1: 0, late + 2: 1},
        scratch_shapes=[pltpu.VMEM((late, rows, columns), half), pltpu.SemaphoreType.DMA((late,))],
        compiler_params=limit(24),
        name="update",
    )(*[near(incoming[d]) for d in arrival[first:]], slots, *state)
    poly = parts[: bool(rest)]
    sent = dict(zip(now, parts[bool(rest) :]))
    if rest:
        parts = pl.pallas_call(
            functools.partial(rest_kernel, arrival),
            in_specs=[VMEM, VMEM],
            out_specs=[VMEM] * len(rest),
            out_shape=[shapes[key] for key in rest],
            compiler_params=limit(16),
            name="rest",
        )(near(poly[0]), near(iterate))
        sent.update(zip(rest, parts))
    held = {}
    for c in range(CHUNKS):
        back = [None] * own
        for k, d in parcels(own, [c]):
            back[d] = swap(sent[k, d], d) if d else sent[k, d]
        for d in PAIRED[c]:
            back[d + 1] = swap(back[d], 1)
        held[c, 0, 0] = pl.pallas_call(
            group_kernel,
            in_specs=[SMEM] + [VMEM] * own,
            out_specs=VMEM,
            out_shape=pltpu.VMEM((count, rows, widths[c]), half),
            compiler_params=limit(4),
        )(owner_table, *map(near, back))
    pairs = [line_pairs(kind, reps, own) for kind in (0, 1)]
    steps = line_steps(reps)
    for stream, step in steps:
        for c in range(CHUNKS):
            behind = held[c, 0, 0] if step == 1 else held[c, stream, step - 1]
            held[c, stream, step] = lax.ppermute(behind, ("rep", "own"), pairs[(stream + step + 1) % 2])
    shape = (reps * count, rows, columns)
    last = [key for key in held if key[1:] == steps[-1]]
    soon = [key for key in held if key not in last]
    updates = place(reps, soon, [held[key] for key in soon], shape, None)
    updates = place(reps, last, [held[key] for key in last], shape, updates)
    return (new_momentum.reshape(1, own * rows, columns), updates)


def solution(mesh):
    in_specs = (P("rep", "own", None), P(("rep", "own"), None, None), P())
    out_specs = (P(("rep", "own"), None, None), P(None, "own", None))
    own, reps = mesh.shape["own"], mesh.shape["rep"]

    def step(grads, momentum, owner_table):
        _, total_rows, columns = grads.shape
        tiled = total_rows % (8 * own) == 0 and columns % (128 * EDGES[-1]) == 0
        if not tiled or own != len(ORDER) + 1 or reps < 3:
            return jax.shard_map(general_body, mesh=mesh, in_specs=in_specs, out_specs=out_specs, check_vma=False)(
                grads, momentum, owner_table
            )

        def body(*args):
            return chunked_body(own, reps, *args)

        mapped = jax.shard_map(body, mesh=mesh, in_specs=in_specs, out_specs=out_specs, check_vma=False)
        return mapped(grads, momentum, owner_table)

    return step
```

```python
import functools
import math

import jax
import jax.numpy as jnp
from jax import lax
from jax.experimental import pallas as pl
from jax.experimental.pallas import tpu as pltpu
from jax.sharding import PartitionSpec as P


ITERS = 2
EDGES = (0, 4, 8)
CHUNKS = len(EDGES) - 1
SOON = 1
PAIRED = ((6,), (2, 4))

DECAY = 0.95
COEF_A = 3.4445
COEF_B = -4.775
COEF_C = 2.0315
EPSILON = 1e-07

ORDER = (6, 7, 2, 4, 3, 5, 1)


VMEM = pl.BlockSpec(memory_space=pltpu.VMEM)
SMEM = pl.BlockSpec(memory_space=pltpu.SMEM)
ANY = pl.BlockSpec(memory_space=pl.ANY)


def limit(mib):
    return pltpu.CompilerParams(vmem_limit_bytes=mib * 2**20)


def spans(columns):
    unit = columns // EDGES[-1]
    return [(unit * a, unit * b) for a, b in zip(EDGES, EDGES[1:])]


def near(x):
    return pltpu.with_memory_space_constraint(x, pltpu.VMEM)


def far(x):
    return pltpu.with_memory_space_constraint(x, pltpu.HBM)


def orthogonalize(blend):
    total = jnp.sqrt(jnp.sum(blend * blend))
    iterate = (blend / (total + EPSILON)).astype(jnp.bfloat16)
    factor = 0.2 * math.sqrt(max(blend.shape[0], blend.shape[1]))
    result = None
    for turn in range(ITERS):
        gram = jnp.dot(iterate, iterate.T, preferred_element_type=jnp.float32).astype(jnp.bfloat16)
        square = jnp.dot(gram, gram, preferred_element_type=jnp.float32)
        poly = (COEF_B * gram.astype(jnp.float32) + COEF_C * square).astype(jnp.bfloat16)
        mixed = COEF_A * iterate.astype(jnp.float32) + jnp.dot(
            poly, iterate, preferred_element_type=jnp.float32
        )
        if turn + 1 < ITERS:
            iterate = mixed.astype(jnp.bfloat16)
        else:
            result = (factor * mixed).astype(jnp.bfloat16)
    return result


def general_body(grads, momentum, owner_table):
    group = lax.axis_index("rep")
    slot_matrix = lax.dynamic_index_in_dim(owner_table, group, 0, keepdims=False)
    matrix_count, _, _ = grads.shape
    is_live = slot_matrix < matrix_count
    clamped = jnp.minimum(slot_matrix, matrix_count - 1)
    half_grads = grads.astype(jnp.bfloat16)
    outgoing = jnp.take(half_grads, clamped, axis=0) * is_live[:, None, None].astype(jnp.bfloat16)
    incoming = lax.all_to_all(outgoing, "own", split_axis=0, concat_axis=1, tiled=True)
    gradient = incoming[0].astype(jnp.float32)
    moment = DECAY * momentum[0].astype(jnp.float32) + gradient
    new_momentum = moment.astype(jnp.bfloat16)[None]
    update = orthogonalize(gradient + DECAY * moment)
    returned = lax.all_to_all(update[None], "own", split_axis=1, concat_axis=0, tiled=True)
    holders = jnp.argsort(slot_matrix)[:matrix_count]
    grouped = jnp.take(returned, holders, axis=0)
    updates = lax.all_gather(grouped, "rep", axis=0, tiled=True)
    return (new_momentum, updates)


def send_order(own):
    return [d for d in ORDER if d < own]


def parcels(own, chunks):
    return [(c, d) for c in chunks for d in range(own) if d & -2 == d or d & -2 not in PAIRED[c]]


def partner(kind, z, reps):
    other = z ^ 1 if kind == 0 else z + 1 if z % 2 else z - 1
    return other if 0 <= other < reps else None


def line_pairs(kind, reps, own):
    pairs = []
    for z in range(reps):
        other = partner(kind, z, reps)
        for o in range(own):
            pairs.append((z * own + o, (z if other is None else other) * own + (o ^ (other is None))))
    return pairs


def source_of(stream, step, z):
    return z + step * (1 - 2 * ((z + stream + step + 1) % 2))


def line_steps(reps):
    return [
        (stream, step)
        for step in range(1, reps)
        for stream in (0, 1)
        if any(0 <= source_of(stream, step, z) < reps for z in range(reps))
    ]


def pack_kernel(table_hbm, grads_hbm, *refs):
    *outs, table, grads, table_sem, sems = refs
    group, me = lax.axis_index("rep"), lax.axis_index("own")
    count = grads.shape[0]
    flights = [pltpu.make_async_copy(table_hbm, table, table_sem)]
    flights += [pltpu.make_async_copy(grads_hbm.at[k], grads.at[k], sems.at[k]) for k in range(count)]
    for flight in flights:
        flight.start()
    flights[0].wait()
    held = [table[group, me ^ d] for d in range(len(outs))]
    for matrix, out in zip(held, outs):

        @pl.when(matrix >= count)
        def _():
            out[...] = jnp.zeros(out.shape, out.dtype)

    for k in range(count):
        flights[k + 1].wait()
        for matrix, out in zip(held, outs):

            @pl.when(matrix == k)
            def _():
                out[...] = grads[k].astype(jnp.bfloat16)


def mix_block(me, d, at, block, momentum, staged, stage_at, new_momentum, sem, blend):
    rows, columns = block.shape
    gradient = block[...].astype(jnp.float32)
    moment = DECAY * momentum[me ^ d].astype(jnp.float32) + gradient
    staged[stage_at] = moment.astype(jnp.bfloat16)
    flight = pltpu.make_async_copy(staged.at[stage_at], new_momentum.at[me ^ d], sem)
    flight.start()
    mix = gradient + DECAY * moment
    blend[at * rows : (at + 1) * rows, :] = mix.astype(jnp.bfloat16)
    return jnp.sum((mix * mix).reshape(rows // 8, 8, columns), axis=0), flight


def mix_kernel(order, first, last, *refs):
    blocks, momentum = refs[: last - first], refs[last - first]
    new_momentum, blend, squares, staged, sems = refs[-5:]
    before = refs[last - first + 3] if first else None
    me = lax.axis_index("own")
    total, flights = (before[...] if first else jnp.zeros(squares.shape, jnp.float32)), []
    for i in range(last - first):
        part, flight = mix_block(
            me, order[first + i], first + i, blocks[i], momentum, staged, i, new_momentum, sems.at[i], blend
        )
        total += part
        flights.append(flight)
    squares[...] = total
    for flight in flights:
        flight.wait()


def finish_chunks(order, chunks, poly, y, at, outs):
    me = lax.axis_index("own")
    rows, edges = y.shape[0] // len(order), spans(y.shape[1])
    factor = 0.2 * math.sqrt(max(y.shape))
    for c in chunks:
        part = y[:, edges[c][0] : edges[c][1]]
        mixed = COEF_A * part.astype(jnp.float32) + jnp.dot(poly, part, preferred_element_type=jnp.float32)
        scaled = (factor * mixed).astype(jnp.bfloat16)
        for i, d in enumerate(order):
            piece = scaled[i * rows : (i + 1) * rows, :]
            if d & -2 in PAIRED[c]:
                outs[at[c, d & -2]][(me ^ d) & 1] = piece
            else:
                outs[at[c, d]][...] = piece


def update_kernel(order, first, *refs):
    late = order[first:]
    blocks, refs = refs[: len(late)], refs[len(late) :]
    momentum, squares = refs[0], refs[3]
    new_momentum, blend, iterate = refs[4:7]
    outs = refs[7 + (SOON < CHUNKS) : -2]
    staged, sems = refs[-2:]
    me = lax.axis_index("own")
    sums, flights = squares[...], []
    for i, d in enumerate(late):
        part, flight = mix_block(me, d, first + i, blocks[i], momentum, staged, i, new_momentum, sems.at[i], blend)
        sums += part
        flights.append(flight)
    scale = 1.0 / (jnp.sqrt(jnp.sum(sums, keepdims=True)) + EPSILON)
    for turn in range(ITERS):
        y = blend[...] if turn == 0 else iterate[...]
        gram32 = lax.dot_general(y, y, (((1,), (1,)), ((), ())), preferred_element_type=jnp.float32)
        if turn == 0:
            gram32 = gram32 * (scale * scale)
        gram = gram32.astype(jnp.bfloat16)
        square = jnp.dot(gram, gram, preferred_element_type=jnp.float32)
        poly = (COEF_B * gram.astype(jnp.float32) + COEF_C * square).astype(jnp.bfloat16)
        if turn + 1 < ITERS:
            for start, stop in spans(y.shape[1]):
                part = y[:, start:stop]
                mixed = COEF_A * part.astype(jnp.float32) + jnp.dot(poly, part, preferred_element_type=jnp.float32)
                if turn == 0:
                    mixed = mixed * scale
                iterate[:, start:stop] = mixed.astype(jnp.bfloat16)
    if SOON < CHUNKS:
        refs[7][...] = poly
    soon = range(SOON)
    finish_chunks(order, soon, poly, iterate, {key: i for i, key in enumerate(parcels(len(order), soon))}, outs)
    for flight in flights:
        flight.wait()


def rest_kernel(order, poly, iterate, *outs):
    chunks = range(SOON, CHUNKS)
    at = {key: i for i, key in enumerate(parcels(len(order), chunks))}
    finish_chunks(order, chunks, poly[...], iterate, at, outs)


def group_kernel(table, *refs):
    *parts, out = refs
    group, me = lax.axis_index("rep"), lax.axis_index("own")
    for d, part in enumerate(parts):
        matrix = table[group, me ^ d]

        @pl.when(matrix < out.shape[0])
        def _():
            out[matrix] = part[me & 1] if len(part.shape) == 3 else part[...]


def place_kernel(reps, where, *refs):
    parts, out, sems = refs[: len(where)], refs[-2], refs[-1]
    group = lax.axis_index("rep")
    count = parts[0].shape[0]
    at_columns = spans(out.shape[2])
    flights = []
    for i, (c, stream, step) in enumerate(where):
        source = group + step * (1 - 2 * lax.rem(group + stream + step + 1, 2))
        here = (source >= 0) & (source < reps)
        at = jnp.clip(source, 0, reps - 1) * count
        start, stop = at_columns[c]
        to = out.at[pl.ds(at, count), :, pl.ds(start, stop - start)]
        flights.append((here, pltpu.make_async_copy(parts[i], to, sems.at[i])))
    for here, copy in flights:
        pl.when(here)(copy.start)
    for here, copy in flights:
        pl.when(here)(copy.wait)


def place(reps, where, parts, shape, out):
    aliases = {} if out is None else {len(where): 0}
    return pl.pallas_call(
        functools.partial(place_kernel, reps, where),
        in_specs=[VMEM] * len(where) + [ANY] * len(aliases),
        out_specs=ANY,
        out_shape=jax.ShapeDtypeStruct(shape, jnp.bfloat16),
        input_output_aliases=aliases,
        scratch_shapes=[pltpu.SemaphoreType.DMA((len(where),))],
        compiler_params=limit(4),
    )(*map(near, parts), *([] if out is None else [out]))


def chunked_body(own, reps, grads, momentum, owner_table):
    count, rows, columns = grads.shape
    widths = [b - a for a, b in spans(columns)]
    half = jnp.bfloat16
    order = send_order(own)
    arrival = [0, order[-1]] + order[:-1]
    stages = [0, own // 2, own - 2] if own > 4 else [0, own - 2]

    def swap(x, d):
        return lax.ppermute(x, "own", [(i, i ^ d) for i in range(own)])

    outgoing = pl.pallas_call(
        pack_kernel,
        in_specs=[ANY, ANY],
        out_specs=[VMEM] * own,
        out_shape=[pltpu.VMEM((rows, columns), half)] * own,
        scratch_shapes=[
            pltpu.SMEM(owner_table.shape, jnp.int32),
            pltpu.VMEM(grads.shape, grads.dtype),
            pltpu.SemaphoreType.DMA(()),
            pltpu.SemaphoreType.DMA((count,)),
        ],
        compiler_params=limit(8),
        name="pack",
    )(far(owner_table), far(grads))
    incoming = {0: outgoing[0]}
    for d in order:
        incoming[d] = swap(outgoing[d], d)
    slots = near(momentum.reshape(own, rows, columns))
    state = []
    for first, last in zip(stages, stages[1:]):
        aliases = {last - first + 1: 0, last - first + 2: 1} if first else {}
        state = pl.pallas_call(
            functools.partial(mix_kernel, arrival, first, last),
            in_specs=[VMEM] * (last - first + 1) + ([ANY, VMEM, VMEM] if first else []),
            out_specs=[ANY, VMEM, VMEM],
            out_shape=[
                jax.ShapeDtypeStruct((own, rows, columns), half),
                pltpu.VMEM((own * rows, columns), half),
                pltpu.VMEM((8, columns), jnp.float32),
            ],
            input_output_aliases=aliases,
            scratch_shapes=[pltpu.VMEM((last - first, rows, columns), half), pltpu.SemaphoreType.DMA((last - first,))],
            compiler_params=limit(8),
        )(*[near(incoming[d]) for d in arrival[first:last]], slots, *state)
        state = [state[0], near(state[1]), near(state[2])]
    first = stages[-1]
    late = own - first
    shapes = {
        (c, d): pltpu.VMEM((2,) * (d in PAIRED[c]) + (rows, widths[c]), half) for c, d in parcels(own, range(CHUNKS))
    }
    now, rest = parcels(own, range(SOON)), parcels(own, range(SOON, CHUNKS))
    new_momentum, _, iterate, *parts = pl.pallas_call(
        functools.partial(update_kernel, arrival, first),
        in_specs=[VMEM] * (late + 1) + [ANY, VMEM, VMEM],
        out_specs=[ANY] + [VMEM] * (2 + bool(rest) + len(now)),
        out_shape=[
            jax.ShapeDtypeStruct((own, rows, columns), half),
            pltpu.VMEM((own * rows, columns), half),
            pltpu.VMEM((own * rows, columns), half),
        ]
        + [pltpu.VMEM((own * rows, own * rows), half)] * bool(rest)
        + [shapes[key] for key in now],
        input_output_aliases={late + 1: 0, late + 2: 1},
        scratch_shapes=[pltpu.VMEM((late, rows, columns), half), pltpu.SemaphoreType.DMA((late,))],
        compiler_params=limit(24),
        name="update",
    )(*[near(incoming[d]) for d in arrival[first:]], slots, *state)
    poly = parts[: bool(rest)]
    sent = dict(zip(now, parts[bool(rest) :]))
    if rest:
        parts = pl.pallas_call(
            functools.partial(rest_kernel, arrival),
            in_specs=[VMEM, VMEM],
            out_specs=[VMEM] * len(rest),
            out_shape=[shapes[key] for key in rest],
            compiler_params=limit(16),
            name="rest",
        )(near(poly[0]), near(iterate))
        sent.update(zip(rest, parts))
    held = {}
    for c in range(CHUNKS):
        back = [None] * own
        for k, d in parcels(own, [c]):
            back[d] = swap(sent[k, d], d) if d else sent[k, d]
        for d in PAIRED[c]:
            back[d + 1] = swap(back[d], 1)
        held[c, 0, 0] = pl.pallas_call(
            group_kernel,
            in_specs=[SMEM] + [VMEM] * own,
            out_specs=VMEM,
            out_shape=pltpu.VMEM((count, rows, widths[c]), half),
            compiler_params=limit(4),
        )(owner_table, *map(near, back))
    pairs = [line_pairs(kind, reps, own) for kind in (0, 1)]
    steps = line_steps(reps)
    for stream, step in steps:
        for c in range(CHUNKS):
            behind = held[c, 0, 0] if step == 1 else held[c, stream, step - 1]
            held[c, stream, step] = lax.ppermute(behind, ("rep", "own"), pairs[(stream + step + 1) % 2])
    shape = (reps * count, rows, columns)
    last = [key for key in held if key[1:] == steps[-1]]
    soon = [key for key in held if key not in last]
    updates = place(reps, soon, [held[key] for key in soon], shape, None)
    updates = place(reps, last, [held[key] for key in last], shape, updates)
    return (new_momentum.reshape(1, own * rows, columns), updates)


def solution(mesh):
    in_specs = (P("rep", "own", None), P(("rep", "own"), None, None), P())
    out_specs = (P(("rep", "own"), None, None), P(None, "own", None))
    own, reps = mesh.shape["own"], mesh.shape["rep"]

    def step(grads, momentum, owner_table):
        _, total_rows, columns = grads.shape
        tiled = total_rows % (8 * own) == 0 and columns % (128 * EDGES[-1]) == 0
        if not tiled or own != len(ORDER) + 1 or reps < 3:
            return jax.shard_map(general_body, mesh=mesh, in_specs=in_specs, out_specs=out_specs, check_vma=False)(
                grads, momentum, owner_table
            )

        def body(*args):
            return chunked_body(own, reps, *args)

        mapped = jax.shard_map(body, mesh=mesh, in_specs=in_specs, out_specs=out_specs, check_vma=False)
        return mapped(grads, momentum, owner_table)

    return step
```

```python
import functools
import math

import jax
import jax.numpy as jnp
from jax import lax
from jax.experimental import pallas as pl
from jax.experimental.pallas import tpu as pltpu
from jax.sharding import PartitionSpec as P


ITERS = 2
EDGES = (0, 4, 8)
CHUNKS = len(EDGES) - 1
SOON = 1
PAIRED = ((6,), (2, 4))

DECAY = 0.95
COEF_A = 3.4445
COEF_B = -4.775
COEF_C = 2.0315
EPSILON = 1e-07

ORDER = (6, 7, 4, 2, 5, 3, 1)


VMEM = pl.BlockSpec(memory_space=pltpu.VMEM)
SMEM = pl.BlockSpec(memory_space=pltpu.SMEM)
ANY = pl.BlockSpec(memory_space=pl.ANY)


def limit(mib):
    return pltpu.CompilerParams(vmem_limit_bytes=mib * 2**20)


def spans(columns):
    unit = columns // EDGES[-1]
    return [(unit * a, unit * b) for a, b in zip(EDGES, EDGES[1:])]


def near(x):
    return pltpu.with_memory_space_constraint(x, pltpu.VMEM)


def far(x):
    return pltpu.with_memory_space_constraint(x, pltpu.HBM)


def orthogonalize(blend):
    total = jnp.sqrt(jnp.sum(blend * blend))
    iterate = (blend / (total + EPSILON)).astype(jnp.bfloat16)
    factor = 0.2 * math.sqrt(max(blend.shape[0], blend.shape[1]))
    result = None
    for turn in range(ITERS):
        gram = jnp.dot(iterate, iterate.T, preferred_element_type=jnp.float32).astype(jnp.bfloat16)
        square = jnp.dot(gram, gram, preferred_element_type=jnp.float32)
        poly = (COEF_B * gram.astype(jnp.float32) + COEF_C * square).astype(jnp.bfloat16)
        mixed = COEF_A * iterate.astype(jnp.float32) + jnp.dot(
            poly, iterate, preferred_element_type=jnp.float32
        )
        if turn + 1 < ITERS:
            iterate = mixed.astype(jnp.bfloat16)
        else:
            result = (factor * mixed).astype(jnp.bfloat16)
    return result


def general_body(grads, momentum, owner_table):
    group = lax.axis_index("rep")
    slot_matrix = lax.dynamic_index_in_dim(owner_table, group, 0, keepdims=False)
    matrix_count, _, _ = grads.shape
    is_live = slot_matrix < matrix_count
    clamped = jnp.minimum(slot_matrix, matrix_count - 1)
    half_grads = grads.astype(jnp.bfloat16)
    outgoing = jnp.take(half_grads, clamped, axis=0) * is_live[:, None, None].astype(jnp.bfloat16)
    incoming = lax.all_to_all(outgoing, "own", split_axis=0, concat_axis=1, tiled=True)
    gradient = incoming[0].astype(jnp.float32)
    moment = DECAY * momentum[0].astype(jnp.float32) + gradient
    new_momentum = moment.astype(jnp.bfloat16)[None]
    update = orthogonalize(gradient + DECAY * moment)
    returned = lax.all_to_all(update[None], "own", split_axis=1, concat_axis=0, tiled=True)
    holders = jnp.argsort(slot_matrix)[:matrix_count]
    grouped = jnp.take(returned, holders, axis=0)
    updates = lax.all_gather(grouped, "rep", axis=0, tiled=True)
    return (new_momentum, updates)


def send_order(own):
    return [d for d in ORDER if d < own]


def parcels(own, chunks):
    return [(c, d) for c in chunks for d in range(own) if d & -2 == d or d & -2 not in PAIRED[c]]


def partner(kind, z, reps):
    other = z ^ 1 if kind == 0 else z + 1 if z % 2 else z - 1
    return other if 0 <= other < reps else None


def line_pairs(kind, reps, own):
    pairs = []
    for z in range(reps):
        other = partner(kind, z, reps)
        for o in range(own):
            pairs.append((z * own + o, (z if other is None else other) * own + (o ^ (other is None))))
    return pairs


def source_of(stream, step, z):
    return z + step * (1 - 2 * ((z + stream + step + 1) % 2))


def line_steps(reps):
    return [
        (stream, step)
        for step in range(1, reps)
        for stream in (0, 1)
        if any(0 <= source_of(stream, step, z) < reps for z in range(reps))
    ]


def pack_kernel(table_hbm, grads_hbm, *refs):
    *outs, table, grads, table_sem, sems = refs
    group, me = lax.axis_index("rep"), lax.axis_index("own")
    count = grads.shape[0]
    flights = [pltpu.make_async_copy(table_hbm, table, table_sem)]
    flights += [pltpu.make_async_copy(grads_hbm.at[k], grads.at[k], sems.at[k]) for k in range(count)]
    for flight in flights:
        flight.start()
    flights[0].wait()
    held = [table[group, me ^ d] for d in range(len(outs))]
    for matrix, out in zip(held, outs):

        @pl.when(matrix >= count)
        def _():
            out[...] = jnp.zeros(out.shape, out.dtype)

    for k in range(count):
        flights[k + 1].wait()
        for matrix, out in zip(held, outs):

            @pl.when(matrix == k)
            def _():
                out[...] = grads[k].astype(jnp.bfloat16)


def mix_block(me, d, at, block, momentum, staged, stage_at, new_momentum, sem, blend):
    rows, columns = block.shape
    gradient = block[...].astype(jnp.float32)
    moment = DECAY * momentum[me ^ d].astype(jnp.float32) + gradient
    staged[stage_at] = moment.astype(jnp.bfloat16)
    flight = pltpu.make_async_copy(staged.at[stage_at], new_momentum.at[me ^ d], sem)
    flight.start()
    mix = gradient + DECAY * moment
    blend[at * rows : (at + 1) * rows, :] = mix.astype(jnp.bfloat16)
    return jnp.sum((mix * mix).reshape(rows // 8, 8, columns), axis=0), flight


def mix_kernel(order, first, last, *refs):
    blocks, momentum = refs[: last - first], refs[last - first]
    new_momentum, blend, squares, staged, sems = refs[-5:]
    before = refs[last - first + 3] if first else None
    me = lax.axis_index("own")
    total, flights = (before[...] if first else jnp.zeros(squares.shape, jnp.float32)), []
    for i in range(last - first):
        part, flight = mix_block(
            me, order[first + i], first + i, blocks[i], momentum, staged, i, new_momentum, sems.at[i], blend
        )
        total += part
        flights.append(flight)
    squares[...] = total
    for flight in flights:
        flight.wait()


def finish_chunks(order, chunks, poly, y, at, outs):
    me = lax.axis_index("own")
    rows, edges = y.shape[0] // len(order), spans(y.shape[1])
    factor = 0.2 * math.sqrt(max(y.shape))
    for c in chunks:
        part = y[:, edges[c][0] : edges[c][1]]
        mixed = COEF_A * part.astype(jnp.float32) + jnp.dot(poly, part, preferred_element_type=jnp.float32)
        scaled = (factor * mixed).astype(jnp.bfloat16)
        for i, d in enumerate(order):
            piece = scaled[i * rows : (i + 1) * rows, :]
            if d & -2 in PAIRED[c]:
                outs[at[c, d & -2]][(me ^ d) & 1] = piece
            else:
                outs[at[c, d]][...] = piece


def update_kernel(order, first, *refs):
    late = order[first:]
    blocks, refs = refs[: len(late)], refs[len(late) :]
    momentum, squares = refs[0], refs[3]
    new_momentum, blend, iterate = refs[4:7]
    outs = refs[7 + (SOON < CHUNKS) : -2]
    staged, sems = refs[-2:]
    me = lax.axis_index("own")
    sums, flights = squares[...], []
    for i, d in enumerate(late):
        part, flight = mix_block(me, d, first + i, blocks[i], momentum, staged, i, new_momentum, sems.at[i], blend)
        sums += part
        flights.append(flight)
    scale = 1.0 / (jnp.sqrt(jnp.sum(sums, keepdims=True)) + EPSILON)
    for turn in range(ITERS):
        y = blend[...] if turn == 0 else iterate[...]
        gram32 = lax.dot_general(y, y, (((1,), (1,)), ((), ())), preferred_element_type=jnp.float32)
        if turn == 0:
            gram32 = gram32 * (scale * scale)
        gram = gram32.astype(jnp.bfloat16)
        square = jnp.dot(gram, gram, preferred_element_type=jnp.float32)
        poly = (COEF_B * gram.astype(jnp.float32) + COEF_C * square).astype(jnp.bfloat16)
        if turn + 1 < ITERS:
            for start, stop in spans(y.shape[1]):
                part = y[:, start:stop]
                mixed = COEF_A * part.astype(jnp.float32) + jnp.dot(poly, part, preferred_element_type=jnp.float32)
                if turn == 0:
                    mixed = mixed * scale
                iterate[:, start:stop] = mixed.astype(jnp.bfloat16)
    if SOON < CHUNKS:
        refs[7][...] = poly
    soon = range(SOON)
    finish_chunks(order, soon, poly, iterate, {key: i for i, key in enumerate(parcels(len(order), soon))}, outs)
    for flight in flights:
        flight.wait()


def rest_kernel(order, poly, iterate, *outs):
    chunks = range(SOON, CHUNKS)
    at = {key: i for i, key in enumerate(parcels(len(order), chunks))}
    finish_chunks(order, chunks, poly[...], iterate, at, outs)


def group_kernel(table, *refs):
    *parts, out = refs
    group, me = lax.axis_index("rep"), lax.axis_index("own")
    for d, part in enumerate(parts):
        matrix = table[group, me ^ d]

        @pl.when(matrix < out.shape[0])
        def _():
            out[matrix] = part[me & 1] if len(part.shape) == 3 else part[...]


def place_kernel(reps, where, *refs):
    parts, out, sems = refs[: len(where)], refs[-2], refs[-1]
    group = lax.axis_index("rep")
    count = parts[0].shape[0]
    at_columns = spans(out.shape[2])
    flights = []
    for i, (c, stream, step) in enumerate(where):
        source = group + step * (1 - 2 * lax.rem(group + stream + step + 1, 2))
        here = (source >= 0) & (source < reps)
        at = jnp.clip(source, 0, reps - 1) * count
        start, stop = at_columns[c]
        to = out.at[pl.ds(at, count), :, pl.ds(start, stop - start)]
        flights.append((here, pltpu.make_async_copy(parts[i], to, sems.at[i])))
    for here, copy in flights:
        pl.when(here)(copy.start)
    for here, copy in flights:
        pl.when(here)(copy.wait)


def place(reps, where, parts, shape, out):
    aliases = {} if out is None else {len(where): 0}
    return pl.pallas_call(
        functools.partial(place_kernel, reps, where),
        in_specs=[VMEM] * len(where) + [ANY] * len(aliases),
        out_specs=ANY,
        out_shape=jax.ShapeDtypeStruct(shape, jnp.bfloat16),
        input_output_aliases=aliases,
        scratch_shapes=[pltpu.SemaphoreType.DMA((len(where),))],
        compiler_params=limit(4),
    )(*map(near, parts), *([] if out is None else [out]))


def chunked_body(own, reps, grads, momentum, owner_table):
    count, rows, columns = grads.shape
    widths = [b - a for a, b in spans(columns)]
    half = jnp.bfloat16
    order = send_order(own)
    arrival = [0, order[-1]] + order[:-1]
    stages = [0, own // 2, own - 2] if own > 4 else [0, own - 2]

    def swap(x, d):
        return lax.ppermute(x, "own", [(i, i ^ d) for i in range(own)])

    outgoing = pl.pallas_call(
        pack_kernel,
        in_specs=[ANY, ANY],
        out_specs=[VMEM] * own,
        out_shape=[pltpu.VMEM((rows, columns), half)] * own,
        scratch_shapes=[
            pltpu.SMEM(owner_table.shape, jnp.int32),
            pltpu.VMEM(grads.shape, grads.dtype),
            pltpu.SemaphoreType.DMA(()),
            pltpu.SemaphoreType.DMA((count,)),
        ],
        compiler_params=limit(8),
        name="pack",
    )(far(owner_table), far(grads))
    incoming = {0: outgoing[0]}
    for d in order:
        incoming[d] = swap(outgoing[d], d)
    slots = near(momentum.reshape(own, rows, columns))
    state = []
    for first, last in zip(stages, stages[1:]):
        aliases = {last - first + 1: 0, last - first + 2: 1} if first else {}
        state = pl.pallas_call(
            functools.partial(mix_kernel, arrival, first, last),
            in_specs=[VMEM] * (last - first + 1) + ([ANY, VMEM, VMEM] if first else []),
            out_specs=[ANY, VMEM, VMEM],
            out_shape=[
                jax.ShapeDtypeStruct((own, rows, columns), half),
                pltpu.VMEM((own * rows, columns), half),
                pltpu.VMEM((8, columns), jnp.float32),
            ],
            input_output_aliases=aliases,
            scratch_shapes=[pltpu.VMEM((last - first, rows, columns), half), pltpu.SemaphoreType.DMA((last - first,))],
            compiler_params=limit(8),
        )(*[near(incoming[d]) for d in arrival[first:last]], slots, *state)
        state = [state[0], near(state[1]), near(state[2])]
    first = stages[-1]
    late = own - first
    shapes = {
        (c, d): pltpu.VMEM((2,) * (d in PAIRED[c]) + (rows, widths[c]), half) for c, d in parcels(own, range(CHUNKS))
    }
    now, rest = parcels(own, range(SOON)), parcels(own, range(SOON, CHUNKS))
    new_momentum, _, iterate, *parts = pl.pallas_call(
        functools.partial(update_kernel, arrival, first),
        in_specs=[VMEM] * (late + 1) + [ANY, VMEM, VMEM],
        out_specs=[ANY] + [VMEM] * (2 + bool(rest) + len(now)),
        out_shape=[
            jax.ShapeDtypeStruct((own, rows, columns), half),
            pltpu.VMEM((own * rows, columns), half),
            pltpu.VMEM((own * rows, columns), half),
        ]
        + [pltpu.VMEM((own * rows, own * rows), half)] * bool(rest)
        + [shapes[key] for key in now],
        input_output_aliases={late + 1: 0, late + 2: 1},
        scratch_shapes=[pltpu.VMEM((late, rows, columns), half), pltpu.SemaphoreType.DMA((late,))],
        compiler_params=limit(24),
        name="update",
    )(*[near(incoming[d]) for d in arrival[first:]], slots, *state)
    poly = parts[: bool(rest)]
    sent = dict(zip(now, parts[bool(rest) :]))
    if rest:
        parts = pl.pallas_call(
            functools.partial(rest_kernel, arrival),
            in_specs=[VMEM, VMEM],
            out_specs=[VMEM] * len(rest),
            out_shape=[shapes[key] for key in rest],
            compiler_params=limit(16),
            name="rest",
        )(near(poly[0]), near(iterate))
        sent.update(zip(rest, parts))
    held = {}
    for c in range(CHUNKS):
        back = [None] * own
        for k, d in parcels(own, [c]):
            back[d] = swap(sent[k, d], d) if d else sent[k, d]
        for d in PAIRED[c]:
            back[d + 1] = swap(back[d], 1)
        held[c, 0, 0] = pl.pallas_call(
            group_kernel,
            in_specs=[SMEM] + [VMEM] * own,
            out_specs=VMEM,
            out_shape=pltpu.VMEM((count, rows, widths[c]), half),
            compiler_params=limit(4),
        )(owner_table, *map(near, back))
    pairs = [line_pairs(kind, reps, own) for kind in (0, 1)]
    steps = line_steps(reps)
    for stream, step in steps:
        for c in range(CHUNKS):
            behind = held[c, 0, 0] if step == 1 else held[c, stream, step - 1]
            held[c, stream, step] = lax.ppermute(behind, ("rep", "own"), pairs[(stream + step + 1) % 2])
    shape = (reps * count, rows, columns)
    last = [key for key in held if key[1:] == steps[-1]]
    soon = [key for key in held if key not in last]
    updates = place(reps, soon, [held[key] for key in soon], shape, None)
    for key in last:
        updates = place(reps, [key], [held[key]], shape, updates)
    return (new_momentum.reshape(1, own * rows, columns), updates)


def solution(mesh):
    in_specs = (P("rep", "own", None), P(("rep", "own"), None, None), P())
    out_specs = (P(("rep", "own"), None, None), P(None, "own", None))
    own, reps = mesh.shape["own"], mesh.shape["rep"]

    def step(grads, momentum, owner_table):
        _, total_rows, columns = grads.shape
        tiled = total_rows % (8 * own) == 0 and columns % (128 * EDGES[-1]) == 0
        if not tiled or own != len(ORDER) + 1 or reps < 3:
            return jax.shard_map(general_body, mesh=mesh, in_specs=in_specs, out_specs=out_specs, check_vma=False)(
                grads, momentum, owner_table
            )

        def body(*args):
            return chunked_body(own, reps, *args)

        mapped = jax.shard_map(body, mesh=mesh, in_specs=in_specs, out_specs=out_specs, check_vma=False)
        return mapped(grads, momentum, owner_table)

    return step
```
